16 devices in a mesh: dp: 4 (over y, z, core), ep: 4 (over x).
Axes of the slice: x: 4, y: 2, z: 1, core: 2. Of those that a mesh axis runs over, the one named last changes fastest.
The devices are a block of a 4x4x8 slice.
Arguments:
- x: bfloat16 [4, 4, 256, 7168], P('dp', 'ep'), parts along dimension 0
- expert: int32 [4, 4, 256, 2], P('dp', 'ep'), parts along dimension 0
- slot: int32 [4, 4, 256, 2], P('dp', 'ep'), parts along dimension 0
- gate: float32 [4, 4, 256, 2], P('dp', 'ep'), parts along dimension 0
- w_gate: bfloat16 [8, 7168, 4864], P('ep')
- w_up: bfloat16 [8, 7168, 4864], P('ep')
- w_down: bfloat16 [8, 4864, 7168], P('ep')
Outputs:
- y: bfloat16 [4, 4, 256, 7168], P('dp', 'ep'), parts along dimension 0
There are 4 independent parts. The reference program is written for one: setup_inputs(seed, part) draws one part's arguments, and reference() takes and returns one part's arrays. A program takes and returns all parts, laid end to end along the dimension named above; an argument that names none is the same for every part.
All inputs are finite; a program needn't handle non-finite values.
Results may differ from the reference program's by a relative error of at most 0.009.
Values are sent between devices in bfloat16 or wider.
A program may use at most 768 MiB of HBM per device.

```python
import jax
import jax.numpy as jnp

MEMBERS = 4
TOKENS = 256
D = 7168
FF = 4864
TOP = 2
EXPERTS = 8
SLOTS = 5 * TOKENS * TOP // (4 * EXPERTS)


def setup_inputs(seed: int = 0, part: int = 0) -> dict:
    own, k1, k2, k3, k4, k5, k6 = jax.random.split(jax.random.key(seed), 7)
    kx, ke, kl, kg = jax.random.split(jax.random.fold_in(own, part), 4)
    devices = (1, MEMBERS)
    place = jax.random.permutation(kl, jnp.arange(EXPERTS, dtype=jnp.uint32))
    slow = ((EXPERTS + (9 * place) % EXPERTS) << ((9 * place) // EXPERTS)) // EXPERTS
    wait = (jax.random.bits(ke, (*devices, TOKENS, EXPERTS), jnp.uint32) >> 10) * slow
    expert = jnp.argsort(wait, axis=-1)[..., :TOP].astype(jnp.int32)
    chosen = jax.nn.one_hot(expert, EXPERTS, dtype=jnp.int32)
    in_line = jnp.cumsum(chosen.reshape(*devices, TOKENS * TOP, EXPERTS), axis=2) - 1
    slot = jnp.sum(in_line.reshape(chosen.shape) * chosen, axis=-1)

    def one(key, rows, columns):
        return (jax.random.normal(key, (rows, columns), jnp.float32) * rows**-0.5).astype(jnp.bfloat16)

    def weights(key, rows, columns):
        return jax.lax.map(lambda k: one(k, rows, columns), jax.random.split(key, EXPERTS))

    return {
        "x": jax.random.normal(kx, (*devices, TOKENS, D), jnp.float32).astype(jnp.bfloat16),
        "expert": expert,
        "slot": slot,
        "gate": jax.nn.softmax(jax.random.normal(kg, expert.shape, jnp.float32)),
        "w_gate": weights(k1, D, FF),
        "w_up": weights(k2, D, FF),
        "w_down": weights(k3, FF, D),
    }


def einsum(form, a, b):
    return jnp.einsum(form, a.astype(jnp.float32), b.astype(jnp.float32))


def reference(x, expert, slot, gate, w_gate, w_up, w_down):
    to_expert = jax.nn.one_hot(expert, EXPERTS, dtype=jnp.bfloat16)
    to_slot = jax.nn.one_hot(slot, SLOTS, dtype=jnp.bfloat16)
    weighted = to_expert * gate[..., None].astype(jnp.bfloat16)
    dispatch = einsum("abtke,abtkc->abtec", to_expert, to_slot).astype(jnp.bfloat16)
    combine = einsum("abtke,abtkc->abtec", weighted, to_slot).astype(jnp.bfloat16)
    z = einsum("abtec,abtd->aebcd", dispatch, x).astype(jnp.bfloat16)
    h = jax.nn.silu(einsum("aebcd,edf->aebcf", z, w_gate))
    h = (h * einsum("aebcd,edf->aebcf", z, w_up)).astype(jnp.bfloat16)
    out = einsum("aebcf,efd->aebcd", h, w_down).astype(jnp.bfloat16)
    y = einsum("abtec,aebcd->abtd", combine, out)
    return y.astype(jnp.bfloat16)
```

```python
import functools

import jax
import jax.numpy as jnp
from jax import lax
from jax.experimental import pallas as pl
from jax.experimental.pallas import tpu as pltpu
from jax.sharding import PartitionSpec as P

F32, BF16 = jnp.float32, jnp.bfloat16
CHUNK = 1024
KC = 512
NC = 256
TN = 256
DOWN = 4


def kernel(
    n, slots, x_hbm, expert_ref, slot_ref, gate_ref, wg_hbm, wu_hbm, wd_hbm, y_hbm,
    x_v, z, stage, back, acc_g, acc_u, h, w_a, w_b, w_c, w_d, wd_v, y_v, sel, comb_l, comb_r,
    x_sem, w_sem, wd_sem, y_sem, d_send, d_recv, c_send, c_recv,
):
    per, depth, ff = wg_hbm.shape
    tokens = x_hbm.shape[0]
    rows = n * slots
    chunks, steps, outs = depth // CHUNK, depth // KC, depth // NC
    per_chunk, outs_chunk = CHUNK // KC, CHUNK // NC
    lo = w_a.shape[1]
    me = lax.axis_index("ep")

    def peer(r):
        return {"ep": lax.rem(me + r, n)}

    def at(i, size):
        return pl.ds(pl.multiple_of(i * size, size), size)

    def x_copy(k):
        return pltpu.make_async_copy(x_hbm.at[:, at(k, CHUNK)], x_v.at[:, at(k, CHUNK)], x_sem.at[k])

    units = (
        (wg_hbm, w_a, acc_g, 0, lo), (wg_hbm, w_b, acc_g, lo, ff - lo),
        (wu_hbm, w_c, acc_u, 0, lo), (wu_hbm, w_d, acc_u, lo, ff - lo),
    )

    def w_copy(u, t):
        src, dst, _, off, width = units[u]
        return pltpu.make_async_copy(
            src.at[lax.div(t, steps), at(lax.rem(t, steps), KC), pl.ds(off, width)], dst, w_sem.at[u]
        )

    def wd_copy(t):
        b = lax.rem(t, DOWN)
        return pltpu.make_async_copy(
            wd_hbm.at[lax.div(t, outs), :, at(lax.rem(t, outs), NC)], wd_v.at[b], wd_sem.at[b]
        )

    def d_copy(e, k, r):
        return pltpu.make_async_remote_copy(
            src_ref=stage.at[pl.ds((r - 1) * slots, slots), at(k, CHUNK)],
            dst_ref=z.at[e, pl.ds(r * slots, slots), at(k, CHUNK)],
            send_sem=d_send.at[k, r - 1], recv_sem=d_recv.at[e, k, r - 1],
            device_id=peer(r), device_id_type=pl.DeviceIdType.MESH,
        )

    def c_copy(e, k, r):
        return pltpu.make_async_remote_copy(
            src_ref=z.at[e, pl.ds(r * slots, slots), at(k, CHUNK)],
            dst_ref=back.at[e, pl.ds((r - 1) * slots, slots), at(k, CHUNK)],
            send_sem=c_send.at[e, k, r - 1], recv_sem=c_recv.at[e, k, r - 1],
            device_id=peer(n - r), device_id_type=pl.DeviceIdType.MESH,
        )

    far_first = (2, 1, 3)

    for k in range(chunks):
        x_copy(k).start()
    for u in range(4):
        w_copy(u, 0).start()
    for t in range(DOWN):
        wd_copy(t).start()
    barrier = pltpu.get_barrier_semaphore()
    for r in range(1, n):
        pl.semaphore_signal(barrier, inc=1, device_id=peer(r), device_id_type=pl.DeviceIdType.MESH)

    ex, sl = expert_ref[...], slot_ref[...]
    owner = lax.shift_right_logical(ex, per.bit_length() - 1)
    place = lax.bitwise_and(owner - me + n, n - 1) * slots + sl
    local = lax.bitwise_and(ex, per - 1)
    gates = gate_ref[...].astype(BF16).astype(F32)
    for e in range(per):
        row = jnp.where(jnp.logical_and(local == e, sl < slots), place, -1)
        lane = lax.broadcasted_iota(jnp.int32, (tokens, rows), 1)
        hit = [row[:, j:j + 1] == lane for j in range(row.shape[1])]
        one = sum(jnp.where(m, 1.0, 0.0) for m in hit)
        sel[e] = one.T.astype(BF16)
        lane = lax.broadcasted_iota(jnp.int32, (tokens, slots), 1)
        comb_l[e] = sum(
            jnp.where(row[:, j:j + 1] == lane, gates[:, j:j + 1], 0.0) for j in range(row.shape[1])
        ).astype(BF16)
        lane = lax.broadcasted_iota(jnp.int32, (tokens, rows - slots), 1) + slots
        comb_r[e] = sum(
            jnp.where(row[:, j:j + 1] == lane, gates[:, j:j + 1], 0.0) for j in range(row.shape[1])
        ).astype(BF16)

    def gather(e, k):
        for i in range(CHUNK // TN):
            cols = pl.ds(pl.multiple_of(k * CHUNK + i * TN, TN), TN)
            part = jnp.dot(sel[e], x_v[:, cols], preferred_element_type=F32).astype(BF16)
            z[e, :slots, cols] = part[:slots]
            stage[:, cols] = part[slots:]

    def send(e, k):
        for r in far_first:
            d_copy(e, k, r).start()

    pl.semaphore_wait(barrier, n - 1)
    x_copy(0).wait()
    gather(0, 0)

    @pl.loop(1, chunks)
    def _(k):
        x_copy(k).wait()
        gather(0, k)
        send(0, k - 1)

    def clear(i, c):
        acc_g[:, at(i, TN)] = jnp.zeros((rows, TN), F32)
        acc_u[:, at(i, TN)] = jnp.zeros((rows, TN), F32)
        return c

    lax.fori_loop(0, ff // TN, clear, 0)
    send(0, chunks - 1)

    def again(k):
        for r in far_first:
            d_copy(0, k, r).wait_send()
        gather(1, k)

    for e in range(per):
        @pl.loop(0, steps)
        def _(c):
            @pl.when(lax.rem(c, per_chunk) == 0)
            def _():
                k = lax.div(c, per_chunk)
                for r in far_first:
                    d_copy(e, k, r).wait_recv()
                if e == 0:
                    @pl.when(k >= 1)
                    def _():
                        again(k - 1)
            cols = at(c, KC)
            t = e * steps + c
            for u, (_, buf, acc, off, width) in enumerate(units):
                w_copy(u, t).wait()
                for i in range(width // TN):
                    here = pl.ds(off + i * TN, TN)
                    acc[:, here] += jnp.dot(
                        z[e, :, cols], buf[:, pl.ds(i * TN, TN)], preferred_element_type=F32
                    )

                @pl.when(t + 1 < per * steps)
                def _():
                    w_copy(u, t + 1).start()
            if e == 0:
                @pl.when(jnp.logical_and(lax.rem(c, per_chunk) == 0, c >= per_chunk))
                def _():
                    send(1, lax.div(c, per_chunk) - 1)

        if e == 0:
            again(chunks - 1)

        def act(i, c):
            cols = at(i, TN)
            h[:, cols] = (jax.nn.silu(acc_g[:, cols]) * acc_u[:, cols]).astype(BF16)
            if e + 1 < per:
                acc_g[:, cols] = jnp.zeros((rows, TN), F32)
                acc_u[:, cols] = jnp.zeros((rows, TN), F32)
            return c

        lax.fori_loop(0, ff // TN, act, 0)
        if e == 0:
            send(1, chunks - 1)

        @pl.loop(0, outs // 2)
        def _(j2):
            for i in range(2):
                j = 2 * j2 + i
                t = e * outs + j
                wd_copy(t).wait()
                part = jnp.dot(h[...], wd_v[lax.rem(t, DOWN)], preferred_element_type=F32)
                z[e, :, at(j, NC)] = part.astype(BF16)

                @pl.when(t + DOWN < per * outs)
                def _():
                    wd_copy(t + DOWN).start()

            j = 2 * j2
            @pl.when(jnp.logical_and(lax.rem(j, outs_chunk) == 0, j > 0))
            def _():
                for r in far_first:
                    c_copy(e, lax.div(j, outs_chunk) - 1, r).start()

        if e + 1 < per:
            for r in far_first:
                c_copy(e, chunks - 1, r).start()

    def y_copy(k):
        b = lax.rem(k, 2)
        return pltpu.make_async_copy(y_v.at[b], y_hbm.at[:, at(k, CHUNK)], y_sem.at[b])

    def finish(k):
        for e in range(per):
            for r in far_first:
                c_copy(e, k, r).wait_recv()

        @pl.when(k >= 2)
        def _():
            y_copy(k - 2).wait()
        for i in range(CHUNK // TN):
            cols = pl.ds(pl.multiple_of(k * CHUNK + i * TN, TN), TN)
            total = 0.0
            for e in range(per):
                total += jnp.dot(comb_l[e], z[e, :slots, cols], preferred_element_type=F32)
                total += jnp.dot(comb_r[e], back[e, :, cols], preferred_element_type=F32)
            y_v[lax.rem(k, 2), :, pl.ds(i * TN, TN)] = total.astype(BF16)
        y_copy(k).start()

    for r in far_first:
        c_copy(per - 1, chunks - 1, r).start()

    @pl.loop(0, chunks)
    def _(k):
        finish(k)

    for k in (chunks - 2, chunks - 1):
        y_copy(k).wait()
    for k in range(chunks):
        for r in far_first:
            d_copy(1, k, r).wait_send()
    for e in range(per):
        for k in range(chunks):
            for r in far_first:
                c_copy(e, k, r).wait_send()


def solution(mesh):
    n = mesh.shape["ep"]

    def layer(x, expert, slot, gate, w_gate, w_up, w_down):
        per, depth, ff = w_gate.shape
        tokens, top = expert.shape[2:]
        slots = 5 * tokens * top // (4 * per * n)
        rows = n * slots
        chunks = depth // CHUNK
        lo = -(-(ff // TN) // 2) * TN
        any_, vmem = pl.BlockSpec(memory_space=pl.ANY), pl.BlockSpec(memory_space=pltpu.VMEM)
        dma = pltpu.SemaphoreType.DMA
        y = pl.pallas_call(
            functools.partial(kernel, n, slots),
            out_shape=jax.ShapeDtypeStruct((tokens, depth), BF16),
            in_specs=[any_, vmem, vmem, vmem, any_, any_, any_],
            out_specs=any_,
            scratch_shapes=[
                pltpu.VMEM((tokens, depth), BF16),
                pltpu.VMEM((per, rows, depth), BF16),
                pltpu.VMEM((rows - slots, depth), BF16),
                pltpu.VMEM((per, rows - slots, depth), BF16),
                pltpu.VMEM((rows, ff), F32),
                pltpu.VMEM((rows, ff), F32),
                pltpu.VMEM((rows, ff), BF16),
                pltpu.VMEM((KC, lo), BF16),
                pltpu.VMEM((KC, ff - lo), BF16),
                pltpu.VMEM((KC, lo), BF16),
                pltpu.VMEM((KC, ff - lo), BF16),
                pltpu.VMEM((DOWN, ff, NC), BF16),
                pltpu.VMEM((2, tokens, CHUNK), BF16),
                pltpu.VMEM((per, rows, tokens), BF16),
                pltpu.VMEM((per, tokens, slots), BF16),
                pltpu.VMEM((per, tokens, rows - slots), BF16),
                dma((chunks,)), dma((4,)), dma((DOWN,)), dma((2,)),
                dma((chunks, n - 1)), dma((per, chunks, n - 1)),
                dma((per, chunks, n - 1)), dma((per, chunks, n - 1)),
            ],
            compiler_params=pltpu.CompilerParams(
                collective_id=0, has_side_effects=True, vmem_limit_bytes=67_000_000
            ),
            cost_estimate=pl.CostEstimate(
                flops=6 * per * rows * depth * ff, bytes_accessed=6 * per * depth * ff, transcendentals=0
            ),
            name="moe",
        )(
            x.reshape(tokens, depth), expert.reshape(tokens, top), slot.reshape(tokens, top),
            gate.reshape(tokens, top), w_gate, w_up, w_down,
        )
        return y.reshape(x.shape)

    token, weight = P("dp", "ep", None, None), P("ep", None, None)
    return jax.shard_map(
        layer, mesh=mesh, in_specs=(token,) * 4 + (weight,) * 3, out_specs=token, check_vma=False
    )
```

```python
import functools

import jax
import jax.numpy as jnp
from jax import lax
from jax.experimental import pallas as pl
from jax.experimental.pallas import tpu as pltpu
from jax.sharding import PartitionSpec as P

F32, BF16 = jnp.float32, jnp.bfloat16
CHUNK = 1024
TOK = 512
KC = 512
TN = 256
AHEAD = 3


def rows_of_choices(n, per, slots, me, ex, sl):
    owner = lax.shift_right_logical(ex, per.bit_length() - 1)
    place = lax.bitwise_and(owner - me + n, n - 1) * slots + sl
    local = lax.bitwise_and(ex, per - 1)
    return [jnp.where(jnp.logical_and(local == e, sl < slots), place, -1) for e in range(per)]


def spread(row, value, rows, first=0):
    tokens = row.shape[1]
    line = lax.broadcasted_iota(jnp.int32, (rows, tokens), 0) + first
    return sum(jnp.where(line == row[j:j + 1], value[j:j + 1], 0.0) for j in range(row.shape[0]))


def exchange_kernel(
    n, slots, x_hbm, expert_ref, slot_ref, gate_ref, wg_hbm, wu_hbm, wd_hbm, out_hbm, y_hbm, comb_hbm,
    x_v, z, stage, acc, h, w_v, sel, comb,
    x_sem, w_sem, l_sem, y_sem, comb_sem, d_send, d_recv, c_send, c_recv,
):
    per, depth, ff = wg_hbm.shape
    tokens, rows = x_hbm.shape[0], n * slots
    chunks, toks, steps = depth // CHUNK, depth // TOK, depth // KC
    assert TOK == KC and 2 * KC == CHUNK and per == 2
    blocks = [(i, min(CHUNK, ff - i * CHUNK)) for i in range(-(-ff // CHUNK))]
    up_first = len(blocks) * KC
    me = lax.axis_index("ep")

    def peer(r):
        return {"ep": lax.rem(me + r, n)}

    def at(i, size):
        return pl.ds(pl.multiple_of(i * size, size), size)

    def x_copy(e, k):
        b = lax.rem(e * toks + k, 2)
        return pltpu.make_async_copy(x_hbm.at[:, at(k, TOK)], x_v.at[b], x_sem.at[b])

    def buf(e, s):
        return lax.rem(e * (steps + chunks) + s, AHEAD)

    def up_copies(e, s):
        b = buf(e, s)
        return [
            pltpu.make_async_copy(
                w.at[e, at(s, KC), pl.ds(i * CHUNK, width)],
                w_v.at[b, pl.ds(first + i * KC, KC), pl.ds(0, width)], w_sem.at[b],
            )
            for w, first in ((wg_hbm, 0), (wu_hbm, up_first))
            for i, width in blocks
        ]

    def down_copy(e, s):
        b = buf(e, s)
        return pltpu.make_async_copy(
            wd_hbm.at[e, :, at(s - steps, CHUNK)], w_v.at[b, pl.ds(0, ff)], w_sem.at[b]
        )

    def refill(e, s):
        @pl.when(s < steps)
        def _():
            for copy in up_copies(e, s):
                copy.start()

        @pl.when(jnp.logical_and(s >= steps, s < steps + chunks))
        def _():
            down_copy(e, s).start()

        if e + 1 < per:
            @pl.when(s >= steps + chunks)
            def _():
                for copy in up_copies(e + 1, s - steps - chunks):
                    copy.start()

    def await_weights(e, s):
        b = buf(e, s)
        whole = w_v.at[b, pl.ds(0, ff)]
        pltpu.make_async_copy(whole, whole, w_sem.at[b]).wait()

    def d_copy(e, k, r):
        return pltpu.make_async_remote_copy(
            src_ref=stage.at[pl.ds((r - 1) * slots, slots), at(k, TOK)],
            dst_ref=z.at[e, pl.ds(r * slots, slots), at(k, TOK)],
            send_sem=d_send.at[k, r - 1], recv_sem=d_recv.at[e, k, r - 1],
            device_id=peer(r), device_id_type=pl.DeviceIdType.MESH,
        )

    def c_copy(e, k, r):
        return pltpu.make_async_remote_copy(
            src_ref=z.at[e, pl.ds(r * slots, slots), at(k, CHUNK)],
            dst_ref=out_hbm.at[e, pl.ds(r * slots, slots), at(k, CHUNK)],
            send_sem=c_send.at[e, k, r - 1], recv_sem=c_recv.at[e, k, r - 1],
            device_id=peer(n - r), device_id_type=pl.DeviceIdType.MESH,
        )

    def l_copy(e, k):
        here = (e, pl.ds(0, slots), at(k, CHUNK))
        return pltpu.make_async_copy(z.at[here], out_hbm.at[here], l_sem.at[e, k])

    far_first = (2, 1, 3)

    for k in range(2):
        x_copy(0, k).start()
    for v in range(AHEAD):
        for copy in up_copies(0, v):
            copy.start()
    barrier = pltpu.get_barrier_semaphore()
    for r in range(1, n):
        pl.semaphore_signal(barrier, inc=1, device_id=peer(r), device_id_type=pl.DeviceIdType.MESH)

    choice_rows = rows_of_choices(n, per, slots, me, expert_ref[...], slot_ref[...])

    def select(e):
        row = choice_rows[e]

        @pl.loop(0, n)
        def _(r):
            sel[e, at(r, slots)] = spread(row, jnp.ones(row.shape, F32), slots, r * slots).astype(BF16)

    select(0)

    def gather(e, k):
        x_copy(e, k).wait()
        b = lax.rem(e * toks + k, 2)
        for i in range(TOK // TN):
            cols = pl.ds(pl.multiple_of(k * TOK + i * TN, TN), TN)
            some = jnp.dot(sel[e], x_v[b, :, pl.ds(i * TN, TN)], preferred_element_type=F32).astype(BF16)
            z[e, :slots, cols] = some[:slots]
            stage[:, cols] = some[slots:]

        @pl.when(k + 2 < toks)
        def _():
            x_copy(e, k + 2).start()

        if e == 0:
            @pl.when(k + 2 >= toks)
            def _():
                x_copy(1, k + 2 - toks).start()

    def send(e, k):
        for r in far_first:
            d_copy(e, k, r).start()

    def give(e, k):
        for r in far_first:
            c_copy(e, k, r).start()
        l_copy(e, k).start()

    pl.semaphore_wait(barrier, n - 1)
    gather(0, 0)
    select(1)
    send(0, 0)

    @pl.loop(1, toks)
    def _(k):
        gather(0, k)

        @pl.when(k > 1)
        def _():
            send(0, k - 1)

    @pl.loop(0, ff // TN)
    def _(i):
        for j in range(2):
            acc[j, :, at(i, TN)] = jnp.zeros((rows, TN), F32)

    send(0, toks - 1)

    gates = gate_ref[...].astype(BF16).astype(F32)
    for e, row in enumerate(choice_rows):
        comb[e] = spread(row, gates, rows).T.astype(BF16)
    comb_copy = pltpu.make_async_copy(comb, comb_hbm, comb_sem)

    def again(k):
        for r in far_first:
            d_copy(0, k, r).wait_send()
        gather(1, k)

    def arrive(e, s):
        for r in far_first:
            d_copy(e, s, r).wait_recv()

    await_weights(0, 0)
    for e in range(per):
        def project(s, i, j):
            block, off = i * TN // CHUNK, i * TN % CHUNK
            return acc[j, :, pl.ds(i * TN, TN)] + jnp.dot(
                z[e, :, at(s, KC)], w_v[buf(e, s), pl.ds(j * up_first + block * KC, KC), pl.ds(off, TN)],
                preferred_element_type=F32,
            )

        @pl.loop(0, steps - 1)
        def _(s):
            arrive(e, s)
            if e == 0:
                @pl.when(s >= 1)
                def _():
                    again(s - 1)
            for i in range(ff // TN):
                for j in range(2):
                    acc[j, :, pl.ds(i * TN, TN)] = project(s, i, j)
            refill(e, s + AHEAD)
            await_weights(e, s + 1)
            if e == 0:
                @pl.when(s >= 1)
                def _():
                    send(1, s - 1)

        arrive(e, steps - 1)
        if e == 0:
            again(toks - 2)
        for i in range(ff // TN):
            gate, up = project(steps - 1, i, 0), project(steps - 1, i, 1)
            h[:, pl.ds(i * TN, TN)] = (jax.nn.silu(gate) * up).astype(BF16)
            for j in range(2):
                if e + 1 < per:
                    acc[j, :, pl.ds(i * TN, TN)] = jnp.zeros((rows, TN), F32)
        refill(e, jnp.int32(steps - 1 + AHEAD))
        await_weights(e, steps)
        if e == 0:
            again(toks - 1)
            send(1, toks - 2)
            send(1, toks - 1)

        @pl.loop(0, chunks)
        def _(p):
            s = steps + p
            for i in range(CHUNK // TN):
                some = jnp.dot(h[...], w_v[buf(e, s), pl.ds(0, ff), pl.ds(i * TN, TN)], preferred_element_type=F32)
                z[e, :, pl.ds(pl.multiple_of(p * CHUNK + i * TN, TN), TN)] = some.astype(BF16)
            refill(e, s + AHEAD)
            if e + 1 < per:
                await_weights(e, s + 1)
            else:
                @pl.when(p + 1 < chunks)
                def _():
                    await_weights(e, s + 1)
            give(e, p)

    comb_copy.start()

    def y_copy(k):
        b = lax.rem(k, AHEAD)
        return pltpu.make_async_copy(
            w_v.at[b, pl.ds(per * rows, tokens)], y_hbm.at[:, at(k, CHUNK)], y_sem.at[b]
        )

    def back_copy(e, k):
        b = lax.rem(k, AHEAD)
        return pltpu.make_async_copy(
            out_hbm.at[e, :, at(k, CHUNK)], w_v.at[b, pl.ds(e * rows, rows)], y_sem.at[b]
        )

    def all_back(k):
        for e in range(per):
            l_copy(e, k).wait()
            for r in far_first:
                c_copy(e, k, r).wait_recv()

    @pl.loop(0, chunks - 1)
    def _(k):
        b = lax.rem(k, AHEAD)
        all_back(k)

        @pl.when(k >= AHEAD)
        def _():
            y_copy(k - AHEAD).wait()
        for e in range(per):
            back_copy(e, k).start()
        for e in range(per):
            back_copy(e, k).wait()
        for i in range(CHUNK // TN):
            cols = pl.ds(i * TN, TN)
            total = 0.0
            for e in range(per):
                total += jnp.dot(comb[e], w_v[b, pl.ds(e * rows, rows), cols], preferred_element_type=F32)
            w_v[b, pl.ds(per * rows, tokens), cols] = total.astype(BF16)
        y_copy(k).start()

    for k in range(chunks - 1 - AHEAD, chunks - 1):
        y_copy(k).wait()
    comb_copy.wait()

    @pl.loop(0, toks)
    def _(k):
        for r in far_first:
            d_copy(1, k, r).wait_send()

    @pl.loop(0, chunks)
    def _(k):
        for e in range(per):
            for r in far_first:
                c_copy(e, k, r).wait_send()

    all_back(chunks - 1)


def last_kernel(comb_hbm, rows_hbm, y_in_hbm, y_hbm, comb, rows_v, y_v, in_sem, out_sem):
    per, _, depth = rows_hbm.shape
    chunks = depth // CHUNK
    last = chunks - 1

    def in_copy(k):
        cols = pl.ds(k * CHUNK, CHUNK)
        if k == last:
            return pltpu.make_async_copy(rows_hbm.at[:, :, cols], rows_v, in_sem.at[k])
        return pltpu.make_async_copy(y_in_hbm.at[:, cols], y_v.at[:, cols], in_sem.at[k])

    def out_copy(k):
        cols = pl.ds(k * CHUNK, CHUNK)
        return pltpu.make_async_copy(y_v.at[:, cols], y_hbm.at[:, cols], out_sem.at[k])

    comb_copy = pltpu.make_async_copy(comb_hbm, comb, in_sem.at[chunks])
    comb_copy.start()
    in_copy(last).start()
    for k in range(last):
        in_copy(k).start()
    comb_copy.wait()
    in_copy(last).wait()
    for i in range(CHUNK // TN):
        cols = pl.ds(i * TN, TN)
        total = 0.0
        for e in range(per):
            total += jnp.dot(comb[e], rows_v[e, :, cols], preferred_element_type=F32)
        y_v[:, pl.ds(last * CHUNK + i * TN, TN)] = total.astype(BF16)
    out_copy(last).start()
    for k in range(last):
        in_copy(k).wait()
        out_copy(k).start()
    for k in range(chunks):
        out_copy(k).wait()


def solution(mesh):
    n = mesh.shape["ep"]

    def layer(x, expert, slot, gate, w_gate, w_up, w_down):
        per, depth, ff = w_gate.shape
        tokens, top = expert.shape[2:]
        slots = 5 * tokens * top // (4 * per * n)
        rows, chunks, toks = n * slots, depth // CHUNK, depth // TOK
        any_, vmem = pl.BlockSpec(memory_space=pl.ANY), pl.BlockSpec(memory_space=pltpu.VMEM)
        dma = pltpu.SemaphoreType.DMA
        expert, slot, gate = (a.reshape(tokens, top).T for a in (expert, slot, gate))
        results, sums, comb = pl.pallas_call(
            functools.partial(exchange_kernel, n, slots),
            out_shape=[
                jax.ShapeDtypeStruct((per, rows, depth), BF16),
                jax.ShapeDtypeStruct((tokens, depth), BF16),
                jax.ShapeDtypeStruct((per, tokens, rows), BF16),
            ],
            in_specs=[any_, vmem, vmem, vmem, any_, any_, any_],
            out_specs=[any_, any_, any_],
            scratch_shapes=[
                pltpu.VMEM((2, tokens, TOK), BF16),
                pltpu.VMEM((per, rows, depth), BF16),
                pltpu.VMEM((rows - slots, depth), BF16),
                pltpu.VMEM((2, rows, ff), F32),
                pltpu.VMEM((rows, ff), BF16),
                pltpu.VMEM((AHEAD, 2 * KC * -(-ff // CHUNK), CHUNK), BF16),
                pltpu.VMEM((per, rows, tokens), BF16),
                pltpu.VMEM((per, tokens, rows), BF16),
                dma((2,)), dma((AHEAD,)), dma((per, chunks)), dma((AHEAD,)), dma(()),
                dma((toks, n - 1)), dma((per, toks, n - 1)),
                dma((per, chunks, n - 1)), dma((per, chunks, n - 1)),
            ],
            compiler_params=pltpu.CompilerParams(
                collective_id=0, has_side_effects=True, vmem_limit_bytes=67_000_000
            ),
            cost_estimate=pl.CostEstimate(
                flops=6 * per * rows * depth * ff, bytes_accessed=6 * per * depth * ff, transcendentals=0
            ),
            name="exchange",
        )(x.reshape(tokens, depth), expert, slot, gate, w_gate, w_up, w_down)
        y = pl.pallas_call(
            last_kernel,
            out_shape=jax.ShapeDtypeStruct((tokens, depth), BF16),
            in_specs=[any_, any_, any_],
            out_specs=any_,
            scratch_shapes=[
                pltpu.VMEM((per, tokens, rows), BF16),
                pltpu.VMEM((per, rows, CHUNK), BF16),
                pltpu.VMEM((tokens, depth), BF16),
                dma((chunks + 1,)), dma((chunks,)),
            ],
            compiler_params=pltpu.CompilerParams(vmem_limit_bytes=60_000_000),
            name="last",
        )(comb, results, sums)
        return y.reshape(x.shape)

    token, weight = P("dp", "ep", None, None), P("ep", None, None)
    return jax.shard_map(
        layer, mesh=mesh, in_specs=(token,) * 4 + (weight,) * 3, out_specs=token, check_vma=False
    )
```

```python
import functools

import jax
import jax.numpy as jnp
from jax import lax
from jax.experimental import pallas as pl
from jax.experimental.pallas import tpu as pltpu
from jax.sharding import PartitionSpec as P

F32, BF16 = jnp.float32, jnp.bfloat16
CHUNK = 1024
TOK = 512
KC = 512
TN = 256
AHEAD = 2


def rows_of_choices(n, per, slots, me, ex, sl):
    owner = lax.shift_right_logical(ex, per.bit_length() - 1)
    place = lax.bitwise_and(owner - me + n, n - 1) * slots + sl
    local = lax.bitwise_and(ex, per - 1)
    return [jnp.where(jnp.logical_and(local == e, sl < slots), place, -1) for e in range(per)]


def spread(row, value, rows, first=0):
    tokens = row.shape[1]
    line = lax.broadcasted_iota(jnp.int32, (rows, tokens), 0) + first
    return sum(jnp.where(line == row[j:j + 1], value[j:j + 1], 0.0) for j in range(row.shape[0]))


def exchange_kernel(
    n, slots, x_hbm, expert_ref, slot_ref, gate_ref, wg_hbm, wu_hbm, wd_hbm, y_hbm,
    x_v, z, stage, back, acc, h, w_v, sel, comb_l, comb_r,
    x_sem, w_sem, y_sem, d_send, d_recv, c_send, c_recv,
):
    per, depth, ff = wg_hbm.shape
    tokens, rows = x_hbm.shape[0], n * slots
    chunks, toks, steps = depth // CHUNK, depth // TOK, depth // KC
    per_chunk = CHUNK // KC
    assert TOK == KC and steps % per_chunk == 0 and per_chunk == 2 and per == 2
    blocks = [(i, min(CHUNK, ff - i * CHUNK)) for i in range(-(-ff // CHUNK))]
    up_first = len(blocks) * KC
    me = lax.axis_index("ep")

    def peer(r):
        return {"ep": lax.rem(me + r, n)}

    def at(i, size):
        return pl.ds(pl.multiple_of(i * size, size), size)

    def x_copy(e, k):
        b = lax.rem(e * toks + k, 2)
        return pltpu.make_async_copy(x_hbm.at[:, at(k, TOK)], x_v.at[b], x_sem.at[b])

    def buf(e, s):
        return lax.rem(e * (steps + chunks) + s, AHEAD)

    def up_copies(e, s):
        b = buf(e, s)
        return [
            pltpu.make_async_copy(
                w.at[e, at(s, KC), pl.ds(i * CHUNK, width)],
                w_v.at[b, pl.ds(first + i * KC, KC), pl.ds(0, width)], w_sem.at[b],
            )
            for w, first in ((wg_hbm, 0), (wu_hbm, up_first))
            for i, width in blocks
        ]

    def down_copy(e, s):
        b = buf(e, s)
        return pltpu.make_async_copy(
            wd_hbm.at[e, :, at(s - steps, CHUNK)], w_v.at[b, pl.ds(0, ff)], w_sem.at[b]
        )

    def refill(e, s):
        @pl.when(s < steps)
        def _():
            for copy in up_copies(e, s):
                copy.start()

        @pl.when(jnp.logical_and(s >= steps, s < steps + chunks))
        def _():
            down_copy(e, s).start()

        if e + 1 < per:
            @pl.when(s >= steps + chunks)
            def _():
                for copy in up_copies(e + 1, s - steps - chunks):
                    copy.start()

    def await_weights(e, s):
        b = buf(e, s)
        whole = w_v.at[b, pl.ds(0, ff)]
        pltpu.make_async_copy(whole, whole, w_sem.at[b]).wait()

    def d_copy(e, k, r):
        return pltpu.make_async_remote_copy(
            src_ref=stage.at[pl.ds((r - 1) * slots, slots), at(k, CHUNK)],
            dst_ref=z.at[e, pl.ds(r * slots, slots), at(k, CHUNK)],
            send_sem=d_send.at[k, r - 1], recv_sem=d_recv.at[e, k, r - 1],
            device_id=peer(r), device_id_type=pl.DeviceIdType.MESH,
        )

    def c_copy(e, k, r):
        return pltpu.make_async_remote_copy(
            src_ref=z.at[e, pl.ds(r * slots, slots), at(k, CHUNK)],
            dst_ref=back.at[e, pl.ds((r - 1) * slots, slots), at(k, CHUNK)],
            send_sem=c_send.at[e, k, r - 1], recv_sem=c_recv.at[e, k, r - 1],
            device_id=peer(n - r), device_id_type=pl.DeviceIdType.MESH,
        )

    far_first = (2, 1, 3)

    for k in range(2):
        x_copy(0, k).start()
    for v in range(AHEAD):
        for copy in up_copies(0, v):
            copy.start()
    barrier = pltpu.get_barrier_semaphore()
    for r in range(1, n):
        pl.semaphore_signal(barrier, inc=1, device_id=peer(r), device_id_type=pl.DeviceIdType.MESH)

    choice_rows = rows_of_choices(n, per, slots, me, expert_ref[...], slot_ref[...])

    def select(e):
        row = choice_rows[e]

        @pl.loop(0, n)
        def _(r):
            sel[e, at(r, slots)] = spread(row, jnp.ones(row.shape, F32), slots, r * slots).astype(BF16)

    select(0)

    def gather(e, k):
        x_copy(e, k).wait()
        b = lax.rem(e * toks + k, 2)
        for i in range(TOK // TN):
            cols = pl.ds(pl.multiple_of(k * TOK + i * TN, TN), TN)
            some = jnp.dot(sel[e], x_v[b, :, pl.ds(i * TN, TN)], preferred_element_type=F32).astype(BF16)
            z[e, :slots, cols] = some[:slots]
            stage[:, cols] = some[slots:]

        @pl.when(k + 2 < toks)
        def _():
            x_copy(e, k + 2).start()

        if e == 0:
            @pl.when(k + 2 >= toks)
            def _():
                x_copy(1, k + 2 - toks).start()

    def send(e, k):
        for r in far_first:
            d_copy(e, k, r).start()

    def give(e, k):
        for r in far_first:
            c_copy(e, k, r).start()

    pl.semaphore_wait(barrier, n - 1)
    def gathers(e, k):
        for i in range(per_chunk):
            gather(e, per_chunk * k + i)

    gathers(0, 0)
    select(1)
    send(0, 0)

    @pl.loop(1, chunks)
    def _(k):
        gathers(0, k)

        @pl.when(k > 1)
        def _():
            send(0, k - 1)

    @pl.loop(0, ff // TN)
    def _(i):
        for j in range(2):
            acc[j, :, at(i, TN)] = jnp.zeros((rows, TN), F32)

    send(0, chunks - 1)

    gates = gate_ref[...].astype(BF16).astype(F32)
    for e, row in enumerate(choice_rows):
        comb_l[e] = spread(row, gates, slots).T.astype(BF16)
        comb_r[e] = spread(row, gates, rows - slots, slots).T.astype(BF16)

    def again(k):
        for r in far_first:
            d_copy(0, k, r).wait_send()
        gathers(1, k)

    def arrive(e, s):
        for r in far_first:
            d_copy(e, s, r).wait_recv()

    await_weights(0, 0)
    for e in range(per):
        def project(s, i, j):
            block, off = i * TN // CHUNK, i * TN % CHUNK
            return acc[j, :, pl.ds(i * TN, TN)] + jnp.dot(
                z[e, :, at(s, KC)], w_v[buf(e, s), pl.ds(j * up_first + block * KC, KC), pl.ds(off, TN)],
                preferred_element_type=F32,
            )

        @pl.loop(0, steps - 1)
        def _(s):
            k = lax.div(s, per_chunk)

            @pl.when(lax.rem(s, per_chunk) == 0)
            def _():
                arrive(e, k)
                if e == 0:
                    @pl.when(s > 0)
                    def _():
                        again(k - 1)
            for i in range(ff // TN):
                for j in range(2):
                    acc[j, :, pl.ds(i * TN, TN)] = project(s, i, j)
            refill(e, s + AHEAD)
            await_weights(e, s + 1)
            if e == 0:
                @pl.when(jnp.logical_and(lax.rem(s, per_chunk) == 0, s > 0))
                def _():
                    send(1, k - 1)

        for i in range(ff // TN):
            gate, up = project(steps - 1, i, 0), project(steps - 1, i, 1)
            h[:, pl.ds(i * TN, TN)] = (jax.nn.silu(gate) * up).astype(BF16)
            for j in range(2):
                if e + 1 < per:
                    acc[j, :, pl.ds(i * TN, TN)] = jnp.zeros((rows, TN), F32)
        refill(e, jnp.int32(steps - 1 + AHEAD))
        await_weights(e, steps)
        if e == 0:
            again(chunks - 1)
            send(1, chunks - 1)

        @pl.loop(0, chunks)
        def _(p):
            s = steps + p
            for i in range(CHUNK // TN):
                some = jnp.dot(h[...], w_v[buf(e, s), pl.ds(0, ff), pl.ds(i * TN, TN)], preferred_element_type=F32)
                z[e, :, pl.ds(pl.multiple_of(p * CHUNK + i * TN, TN), TN)] = some.astype(BF16)
            refill(e, s + AHEAD)
            if e + 1 < per:
                await_weights(e, s + 1)
            else:
                @pl.when(p + 1 < chunks)
                def _():
                    await_weights(e, s + 1)
            give(e, p)

    def y_copy(k):
        b = lax.rem(k, AHEAD)
        return pltpu.make_async_copy(w_v.at[b, pl.ds(0, tokens)], y_hbm.at[:, at(k, CHUNK)], y_sem.at[b])

    @pl.loop(0, chunks)
    def _(k):
        b = lax.rem(k, AHEAD)
        for e in range(per):
            for r in far_first:
                c_copy(e, k, r).wait_recv()

        @pl.when(k >= AHEAD)
        def _():
            y_copy(k - AHEAD).wait()
        for i in range(CHUNK // TN):
            cols = pl.ds(pl.multiple_of(k * CHUNK + i * TN, TN), TN)
            total = 0.0
            for e in range(per):
                total += jnp.dot(comb_l[e], z[e, :slots, cols], preferred_element_type=F32)
                total += jnp.dot(comb_r[e], back[e, :, cols], preferred_element_type=F32)
            w_v[b, :tokens, pl.ds(i * TN, TN)] = total.astype(BF16)
        y_copy(k).start()

    for k in range(chunks - AHEAD, chunks):
        y_copy(k).wait()

    @pl.loop(0, chunks)
    def _(k):
        for r in far_first:
            d_copy(1, k, r).wait_send()
        for e in range(per):
            for r in far_first:
                c_copy(e, k, r).wait_send()


def copy_kernel(y_in_hbm, y_hbm, y_v, in_sem, out_sem):
    chunks = y_v.shape[1] // CHUNK

    def in_copy(k):
        cols = pl.ds(k * CHUNK, CHUNK)
        return pltpu.make_async_copy(y_in_hbm.at[:, cols], y_v.at[:, cols], in_sem.at[k])

    def out_copy(k):
        cols = pl.ds(k * CHUNK, CHUNK)
        return pltpu.make_async_copy(y_v.at[:, cols], y_hbm.at[:, cols], out_sem.at[k])

    for k in range(chunks):
        in_copy(k).start()
    for k in range(chunks):
        in_copy(k).wait()
        out_copy(k).start()
    for k in range(chunks):
        out_copy(k).wait()


def solution(mesh):
    n = mesh.shape["ep"]

    def layer(x, expert, slot, gate, w_gate, w_up, w_down):
        per, depth, ff = w_gate.shape
        tokens, top = expert.shape[2:]
        slots = 5 * tokens * top // (4 * per * n)
        rows, chunks = n * slots, depth // CHUNK
        any_, vmem = pl.BlockSpec(memory_space=pl.ANY), pl.BlockSpec(memory_space=pltpu.VMEM)
        dma = pltpu.SemaphoreType.DMA
        expert, slot, gate = (a.reshape(tokens, top).T for a in (expert, slot, gate))
        sums = pl.pallas_call(
            functools.partial(exchange_kernel, n, slots),
            out_shape=jax.ShapeDtypeStruct((tokens, depth), BF16),
            in_specs=[any_, vmem, vmem, vmem, any_, any_, any_],
            out_specs=any_,
            scratch_shapes=[
                pltpu.VMEM((2, tokens, TOK), BF16),
                pltpu.VMEM((per, rows, depth), BF16),
                pltpu.VMEM((rows - slots, depth), BF16),
                pltpu.VMEM((per, rows - slots, depth), BF16),
                pltpu.VMEM((2, rows, ff), F32),
                pltpu.VMEM((rows, ff), BF16),
                pltpu.VMEM((AHEAD, 2 * KC * -(-ff // CHUNK), CHUNK), BF16),
                pltpu.VMEM((per, rows, tokens), BF16),
                pltpu.VMEM((per, tokens, slots), BF16),
                pltpu.VMEM((per, tokens, rows - slots), BF16),
                dma((2,)), dma((AHEAD,)), dma((AHEAD,)),
                dma((chunks, n - 1)), dma((per, chunks, n - 1)),
                dma((per, chunks, n - 1)), dma((per, chunks, n - 1)),
            ],
            compiler_params=pltpu.CompilerParams(
                collective_id=0, has_side_effects=True, vmem_limit_bytes=67_000_000
            ),
            cost_estimate=pl.CostEstimate(
                flops=6 * per * rows * depth * ff, bytes_accessed=6 * per * depth * ff, transcendentals=0
            ),
            name="exchange",
        )(x.reshape(tokens, depth), expert, slot, gate, w_gate, w_up, w_down)
        y = pl.pallas_call(
            copy_kernel,
            out_shape=jax.ShapeDtypeStruct((tokens, depth), BF16),
            in_specs=[any_],
            out_specs=any_,
            scratch_shapes=[pltpu.VMEM((tokens, depth), BF16), dma((chunks,)), dma((chunks,))],
            compiler_params=pltpu.CompilerParams(vmem_limit_bytes=60_000_000),
            name="copy",
        )(sums)
        return y.reshape(x.shape)

    token, weight = P("dp", "ep", None, None), P("ep", None, None)
    return jax.shard_map(
        layer, mesh=mesh, in_specs=(token,) * 4 + (weight,) * 3, out_specs=token, check_vma=False
    )
```
